32 devices in a mesh: row: 8 (over y, x, core), col: 4 (over z).
Axes of the slice: x: 2, y: 2, z: 4, core: 2. Of those that a mesh axis runs over, the one named last changes fastest.
Arguments:
- tiles: float32 [8, 4, 4, 512, 512], P('row', 'col'), may hold values from 0 to 16777212, as said below
- tile_index: int32 [8, 4, 4, 2], P('row', 'col'), may hold values from 0 to 3, as said below
- tile_count: int32 [8, 4], P('row', 'col'), may hold values from 0 to 4, as said below
- iterate: float32 [8192, 32], P(('row', 'col')), may hold values from 0 to 16777212, as said below
- basis: float32 [8192, 32], P(('row', 'col')), may hold values from 0 to 16777212, as said below
- coefficients: float32 [256, 32, 32], P(('row', 'col')), may hold values from 0 to 16777212, as said below
- start_degree: int32 [1], replicated, may hold values from 1 to 255
Outputs:
- scaled_iterate: float32 [8192, 32], P(('row', 'col'))
The draws below stay inside these ranges and needn't reach their ends.
Inputs may be any that keep to these rules, and one draw needn't show every extreme that they name: `tiles`: integers 0 to 16777212. `iterate`: integers 0 to 16777212. `basis`: integers 0 to 16777212. `coefficients`: integers 0 to 16777212. tile_index[..., 0] lies in 0 to 1 and tile_index[..., 1] in 0 to 3; the 4 slots of one device name distinct tiles, unoccupied slots included; unoccupied slots hold arbitrary entries. `tile_count`: some device has 4 occupied slots.
All inputs are finite; a program needn't handle non-finite values.
Results may differ from the reference program's by a relative error of at most 0.0003.
Values sent between devices are 32-bit elements; how exact they have to be, the bound alone decides.
A program may use at most 64 MiB of HBM per device.

```python
import jax
import jax.numpy as jnp
from jax import lax

BW = 32
TILE = 512
ROWS_DEV = 256
TD = 4
STEPS = 2
ORDER = 8192
TR = 2
TC = 4
DEG = 256
N_ROW = 8
N_COL = 4


def draw_residues(key, shape):
    return jax.random.randint(key, shape, 0, 16777213).astype(jnp.float32)


def layout_pick(key):
    pick_key = jax.random.fold_in(key, 21)
    block_key, tile_key, column_key = jax.random.split(pick_key, 3)
    empty_col = jax.random.randint(column_key, (), 0, TC).astype(jnp.int32)
    empty_lo = (TILE * empty_col // ROWS_DEV).astype(jnp.int32)
    empty_hi = ((TILE * (empty_col + 1) - 1) // ROWS_DEV).astype(jnp.int32)
    kept_rows = (N_ROW - (empty_hi - empty_lo + 1)).astype(jnp.int32)
    offset = jax.random.randint(block_key, (), 0, kept_rows).astype(jnp.int32)
    chosen_block = ((empty_hi + 1 + offset) % N_ROW).astype(jnp.int32)
    chosen_tile = jax.random.randint(tile_key, (), 0, TR).astype(jnp.int32)
    return (chosen_block, chosen_tile, empty_col, empty_lo, empty_hi, kept_rows)


def empty_rows(empty_lo, empty_hi):
    row_ids = jnp.arange(N_ROW)
    return (row_ids >= empty_lo) & (row_ids <= empty_hi)


def draw_tiles(key, part):
    chosen_block, chosen_tile, empty_col, empty_lo, empty_hi, kept_rows = layout_pick(key)
    raw_tiles = jax.random.randint(jax.random.fold_in(key, 11), (N_ROW, N_COL, TD, TILE, TILE), 0, 16777213).astype(jnp.int32)
    slab = raw_tiles[chosen_block, :, 0]
    partial_total = jnp.sum(slab[:N_COL - 1], axis=0) % 16777213
    closing = ((16777213 - partial_total) % 16777213).astype(jnp.int32)
    slab = slab.at[N_COL - 1].set(closing)
    raw_tiles = raw_tiles.at[chosen_block, :, 0].set(slab)
    return raw_tiles.astype(jnp.float32)


def draw_tile_index(key, part):
    chosen_block, chosen_tile, empty_col, empty_lo, empty_hi, kept_rows = layout_pick(key)
    cells = TR * TC
    devices_all = N_ROW * N_COL
    base_key = jax.random.fold_in(key, 12)
    list_key, short_key, pick_key = jax.random.split(base_key, 3)
    key_list = jax.random.split(list_key, devices_all)
    scores = jax.vmap(lambda device_key: jax.random.permutation(device_key, cells))(key_list).astype(jnp.int32)
    in_block = jnp.arange(devices_all) // N_COL == chosen_block
    in_row = jnp.arange(cells) // TC == chosen_tile
    pushed = scores + cells * (in_block[:, None] & in_row[None, :]).astype(jnp.int32)
    ordered = jnp.argsort(pushed, axis=1, stable=True)[:, :TD].astype(jnp.int32)
    cancel_cell = (chosen_tile * TC + empty_col).astype(jnp.int32)
    leading = jnp.broadcast_to(cancel_cell, (devices_all, 1)).astype(jnp.int32)
    shifted = jnp.concatenate([leading, ordered[:, :TD - 1]], axis=1)
    cell_ids = jnp.where(in_block[:, None], shifted, ordered)
    middle = 1 + jax.random.permutation(short_key, cells - 2)[:TD - 2]
    special = jnp.concatenate([jnp.array([cells - 1, 0], jnp.int32), middle.astype(jnp.int32)])
    chosen = empty_lo * N_COL + jax.random.randint(pick_key, (), 0, N_COL).astype(jnp.int32)
    picked = jnp.arange(devices_all)[:, None] == chosen
    cell_ids = jnp.where(picked, special[None, :], cell_ids)
    tile_slots = jnp.stack([cell_ids // TC, cell_ids % TC], axis=-1).astype(jnp.int32)
    return tile_slots.reshape(N_ROW, N_COL, TD, 2)


def draw_tile_count(key, part):
    chosen_block, chosen_tile, empty_col, empty_lo, empty_hi, kept_rows = layout_pick(key)
    count_key, pick_key, column_key = jax.random.split(jax.random.fold_in(key, 13), 3)
    device_ids = jnp.arange(N_ROW * N_COL)
    slot_counts = jax.random.randint(count_key, (N_ROW * N_COL,), 1, TD + 1)
    busy_row = (empty_hi + 1 + jax.random.randint(pick_key, (), 0, kept_rows).astype(jnp.int32)) % N_ROW
    busiest = busy_row * N_COL + jax.random.randint(column_key, (), 0, N_COL).astype(jnp.int32)
    slot_counts = jnp.where(device_ids == busiest, TD, slot_counts)
    silent_rows = empty_rows(empty_lo, empty_hi)
    slot_counts = jnp.where(silent_rows[device_ids // N_COL], 0, slot_counts)
    return slot_counts.reshape(N_ROW, N_COL).astype(jnp.int32)


def draw_iterate(key, part):
    return draw_residues(jax.random.fold_in(key, 14), (ORDER, BW))


def draw_basis(key, part):
    chosen_block, chosen_tile, empty_col, empty_lo, empty_hi, kept_rows = layout_pick(key)
    fresh = draw_residues(jax.random.fold_in(key, 15), (ORDER, BW)).reshape(N_ROW, N_COL, ROWS_DEV, BW)
    repeated = jnp.broadcast_to(fresh[:, :1], fresh.shape)
    late_rows = empty_rows(empty_lo, empty_hi)[:, None, None, None]
    shaped = jnp.where(late_rows, repeated, fresh).reshape(ORDER, BW)
    row_ids = jnp.arange(ORDER)
    first_row = chosen_block * (ROWS_DEV * N_COL) + chosen_tile * TILE
    silent = (row_ids >= first_row) & (row_ids < first_row + TILE)
    return jnp.where(silent[:, None], jnp.float32(0.0), shaped).astype(jnp.float32)


def draw_coefficients(key, part):
    return draw_residues(jax.random.fold_in(key, 16), (DEG, BW, BW))


def setup_inputs(seed: int = 0) -> dict:
    splits = jax.random.split(jax.random.key(seed), 8)
    return {
        "tiles": draw_tiles(jax.random.fold_in(splits[7], 71), 0),
        "tile_index": draw_tile_index(jax.random.fold_in(splits[7], 71), 0),
        "tile_count": draw_tile_count(jax.random.fold_in(splits[7], 71), 0),
        "iterate": draw_iterate(jax.random.fold_in(splits[7], 71), 0),
        "basis": draw_basis(jax.random.fold_in(splits[7], 71), 0),
        "coefficients": draw_coefficients(jax.random.fold_in(splits[7], 71), 0),
        "start_degree": jax.random.randint(splits[6], (1,), STEPS - 1, DEG).astype(jnp.int32),
    }


PRIME = 16777213
RADIX = 16777216


def fold_word(value):
    value = value % RADIX + 3 * (value // RADIX)
    return jnp.where(value >= PRIME, value - PRIME, value)


def add_mod(first, second):
    total = first + second
    return jnp.where(total >= PRIME, total - PRIME, total)


def shift_mod(value, shift):
    while shift > 0:
        amount = min(shift, 7)
        value = fold_word(value * (2 ** amount))
        shift = shift - amount
    return value


def split_limbs(values, bits, count):
    whole = values.astype(jnp.int32)
    return [((whole // (2 ** (bits * place))) % (2 ** bits)).astype(jnp.bfloat16) for place in range(count)]


def combine_limbs(product, left_bits, right_bits, width):
    whole = product.astype(jnp.int32)
    total = None
    for left in range(whole.shape[-3]):
        for right in range(whole.shape[-1] // width):
            piece = whole[..., left, :, right * width:(right + 1) * width]
            term = shift_mod(piece, left_bits * left + right_bits * right)
            total = term if total is None else add_mod(total, term)
    return total


def reference(tiles, tile_index, tile_count, iterate, basis, coefficients, start_degree):
    basis_limbs = jnp.stack(split_limbs(basis, 8, 3)).astype(jnp.float32)
    current = iterate
    for step in range(STEPS):
        coef = lax.dynamic_index_in_dim(coefficients, start_degree[0] - step, 0, keepdims=False)
        coef_limbs = jnp.concatenate(split_limbs(coef, 8, 3), axis=1).astype(jnp.float32)
        grouped = current.reshape(N_ROW, N_COL, ROWS_DEV, BW).transpose(1, 0, 2, 3).reshape(N_COL, N_ROW * ROWS_DEV, BW)
        column_limbs = jnp.concatenate(split_limbs(grouped, 6, 4), axis=2).astype(jnp.float32)

        def one_block(row_id):
            block = tiles[row_id]
            tile_limbs = jnp.stack(split_limbs(block, 8, 3), axis=2).astype(jnp.float32)
            slots_here = tile_index[row_id]

            def windows_of(limb_rows, column_ids):
                return jax.vmap(lambda column: lax.dynamic_slice_in_dim(limb_rows, column * TILE, TILE, 0))(column_ids)

            windows = jax.vmap(windows_of)(column_limbs, slots_here[:, :, 1])
            product = jnp.einsum("jtlik,jtkc->jtlic", tile_limbs, windows, precision=lax.Precision.HIGHEST)
            residues = combine_limbs(product, 8, 6, BW)
            used = jnp.arange(TD)[None, :] < tile_count[row_id][:, None]
            kept = jnp.where(used[:, :, None, None], residues, 0)
            match = slots_here[:, :, 0][:, :, None] == jnp.arange(TR)[None, None, :]
            partial_value = jnp.sum(jnp.where(match[:, :, :, None, None], kept[:, :, None], 0), axis=(0, 1)) % PRIME
            return partial_value.reshape(TR * TILE, BW)

        products = lax.map(one_block, jnp.arange(N_ROW))
        local = products.reshape(ORDER, BW)
        basis_term = combine_limbs(jnp.einsum("lrk,kc->lrc", basis_limbs, coef_limbs, precision=lax.Precision.HIGHEST), 8, 8, BW)
        current = add_mod(local, basis_term).astype(jnp.float32)
    return current / PRIME
```

```python
import functools

import jax
import jax.numpy as jnp
from jax import lax
from jax.experimental import pallas as pl
from jax.experimental.pallas import tpu as pltpu
from jax.sharding import PartitionSpec as P

STEPS = 2
PRIME = 16777213
HALF = 8388608.0
MAGIC = 12582912.0
LEFT = 3
RIGHT = 4
MESH = pl.DeviceIdType.MESH


def nearest(value):
    return (value + MAGIC) - MAGIC


def digits(value, bits, count):
    out = []
    for place in range(count - 1, 0, -1):
        top = nearest(value * (2.0 ** (-bits * place)))
        value = value - top * (2.0 ** (bits * place))
        out.append(top)
    out.append(value)
    return out[::-1]


def centred(value):
    return value - jnp.where(value > HALF, float(PRIME), 0.0)


def shrink(value):
    high = (value + 2**23) >> 24
    return value - (high << 24) + 3 * high


def shifted(value, shift):
    if shift == 0:
        return value
    return ((value & (2 ** (24 - shift) - 1)) << shift) + 3 * (value >> (24 - shift))


def kernel(
    n_row, n_col, index_ref, count_ref, degree_ref, tiles_ref, iterate_ref, basis_ref, coef_ref,
    out_ref, tbuf, abuf, gbuf, lbuf, wbuf, pbuf, rbuf, cur, bterm, csrc, crecv, fsum, frecv,
    tile_sem, ag_send, ag_recv, rs_send, rs_recv, ca_send, ca_recv, cb_send, cb_recv,
):
    me_row = lax.axis_index("row")
    me_col = lax.axis_index("col")
    slots, tile, _ = tiles_ref.shape
    width, rows_dev = iterate_ref.shape
    per_tile = tile // rows_dev
    block_rows = n_col // per_tile
    band = RIGHT * width

    def row_peer(d):
        return lax.rem(me_row + d, n_row)

    def col_peer(d):
        return lax.rem(me_col + d, n_col)

    loads = [
        pltpu.make_async_copy(tiles_ref.at[t], tbuf.at[t], tile_sem.at[t]) for t in range(slots)
    ]
    for load in loads:
        load.start()

    barrier = pltpu.get_barrier_semaphore()

    @pl.loop(1, n_row)
    def _(d):
        pl.semaphore_signal(barrier, inc=1, device_id={"row": row_peer(d)}, device_id_type=MESH)

    @pl.loop(1, n_col)
    def _(d):
        pl.semaphore_signal(barrier, inc=1, device_id={"col": col_peer(d)}, device_id_type=MESH)

    per_device = coef_ref.shape[0]
    me = me_row * n_col + me_col
    held = []
    for step in range(STEPS):
        wanted = degree_ref[0] - step
        matrix = coef_ref[lax.rem(wanted + per_device, per_device)]
        matrix = jnp.where(lax.div(wanted, per_device) == me, matrix, 0.0)
        held += [matrix[: width // 2], matrix[width // 2 :]]
    csrc[...] = jnp.concatenate(held, axis=1)

    pl.semaphore_wait(barrier, n_row + n_col - 2)

    def gather_copy(step, d, slot):
        return pltpu.make_async_remote_copy(
            src_ref=iterate_ref if step == 0 else cur,
            dst_ref=gbuf.at[step, slot],
            send_sem=ag_send.at[step, d],
            recv_sem=ag_recv.at[step, slot],
            device_id={"row": row_peer(d)},
            device_id_type=MESH,
        )

    def scatter_copy(step, chunk, slot, peer):
        return pltpu.make_async_remote_copy(
            src_ref=pbuf.at[step, chunk],
            dst_ref=rbuf.at[step, slot],
            send_sem=rs_send.at[step, chunk],
            recv_sem=rs_recv.at[step, slot],
            device_id={"col": peer},
            device_id_type=MESH,
        )

    def coef_col_copy(d, slot):
        return pltpu.make_async_remote_copy(
            src_ref=csrc,
            dst_ref=crecv.at[slot],
            send_sem=ca_send.at[d],
            recv_sem=ca_recv.at[slot],
            device_id={"col": col_peer(d)},
            device_id_type=MESH,
        )

    def coef_row_copy(d, slot):
        return pltpu.make_async_remote_copy(
            src_ref=fsum,
            dst_ref=frecv.at[slot],
            send_sem=cb_send.at[d],
            recv_sem=cb_recv.at[slot],
            device_id={"row": row_peer(d)},
            device_id_type=MESH,
        )

    def put_limbs(value, slot):
        parts = digits(centred(value), 6, RIGHT)
        lbuf[slot] = jnp.concatenate(parts, axis=0).astype(jnp.bfloat16)

    def split_tiles():
        rows = 64
        for t in range(slots):
            loads[t].wait()

            @pl.loop(0, tile // rows)
            def _(i, t=t):
                at = pl.ds(pl.multiple_of(i * rows, rows), rows)
                parts = digits(tbuf[t, at, :], 8, LEFT)
                for place in range(LEFT):
                    abuf[place, at, t * tile : (t + 1) * tile] = parts[place].astype(jnp.bfloat16)

    def basis_terms():
        @pl.loop(1, n_row)
        def _(d):
            src = lax.rem(me_row - d + n_row, n_row)
            coef_row_copy(d, src).wait_recv()

        def add(d, total):
            return total + frecv[lax.rem(me_row + d, n_row)]

        coefs = lax.fori_loop(1, n_row, add, fsum[...])
        basis_digits = [x.astype(jnp.bfloat16) for x in digits(centred(basis_ref[...]), 8, 3)]
        for step in range(STEPS):
            low = coefs[:, (2 * step) * width : (2 * step + 1) * width]
            high = coefs[:, (2 * step + 1) * width : (2 * step + 2) * width]
            matrix = centred(jnp.concatenate([low, high], axis=0))
            parts = [x.T.astype(jnp.bfloat16) for x in digits(matrix, 8, 3)]
            left = jnp.concatenate(parts, axis=0)
            sums = [None] * 5
            for place in range(3):
                product = jnp.dot(left, basis_digits[place], preferred_element_type=jnp.float32)
                for other in range(3):
                    piece = product[other * width : (other + 1) * width]
                    old = sums[place + other]
                    sums[place + other] = piece if old is None else old + piece
            sums = [x.astype(jnp.int32) for x in sums]
            total = sums[0] + 3 * sums[3] + ((sums[1] + 3 * sums[4]) << 8)
            total = total + shifted(sums[2], 16)
            bterm[step] = shrink(total)

    for step in range(STEPS):
        if step == 0:

            @pl.loop(1, n_col)
            def _(d):
                coef_col_copy(d, me_col).start()

        @pl.loop(1, n_row)
        def _(d, step=step):
            gather_copy(step, d, me_row).start()

        put_limbs((iterate_ref if step == 0 else cur)[...], me_row)
        if step == 0:
            split_tiles()

            def add_col(d, total):
                src = lax.rem(me_col - d + n_col, n_col)
                coef_col_copy(d, src).wait_recv()
                return total + crecv[src]

            fsum[...] = lax.fori_loop(1, n_col, add_col, csrc[...])

        @pl.loop(1, n_row)
        def _(d, step=step):
            src = lax.rem(me_row - d + n_row, n_row)
            gather_copy(step, d, src).wait_recv()
            put_limbs(gbuf[step, src], src)

        if step == 0:

            @pl.loop(1, n_row)
            def _(d):
                coef_row_copy(d, me_row).start()

        for t in range(slots):
            column = index_ref[t, 1]
            used = t < count_ref[0, 0]
            for part in range(per_tile):
                window = lbuf[column * per_tile + part]
                at = t * tile + part * rows_dev
                for a in range(block_rows):
                    keep = jnp.where(used & (index_ref[t, 0] == a), 1.0, 0.0).astype(jnp.bfloat16)
                    wbuf[a * band : (a + 1) * band, at : at + rows_dev] = window * keep

        for part in range(per_tile):
            rows = slice(part * rows_dev, (part + 1) * rows_dev)
            whole = [
                lax.dot_general(
                    wbuf[...],
                    abuf[place, rows, :],
                    (((1,), (1,)), ((), ())),
                    preferred_element_type=jnp.float32,
                ).astype(jnp.int32)
                for place in range(LEFT)
            ]
            for a in range(block_rows):
                total = None
                for j in range(RIGHT):
                    at = slice(a * band + j * width, a * band + (j + 1) * width)
                    p0, p1, p2 = [x[at] for x in whole]
                    term = p0 + ((p1 & 0xFFFF) << 8) + ((p2 & 0xFF) << 16)
                    term = shifted(term + 3 * ((p1 >> 16) + (p2 >> 8)), 6 * j)
                    total = term if total is None else total + term
                chunk = a * per_tile + part
                pbuf[step, chunk] = shrink(total).astype(jnp.float32)

                @pl.when(me_col != chunk)
                def _(step=step, chunk=chunk):
                    scatter_copy(step, chunk, me_col, chunk).start()

        if step == 0:
            basis_terms()

        def add_chunk(d, total, step=step):
            src = lax.rem(me_col - d + n_col, n_col)
            scatter_copy(step, src, src, src).wait_recv()
            return total + rbuf[step, src].astype(jnp.int32)

        start = bterm[step] + pbuf[step, me_col].astype(jnp.int32)
        value = shrink(lax.fori_loop(1, n_col, add_chunk, start))
        if step < STEPS - 1:
            cur[...] = value.astype(jnp.float32)
        else:
            value = jnp.where(value < 0, value + PRIME, value)
            out_ref[...] = value.astype(jnp.float32) / float(PRIME)

    @pl.loop(1, n_row)
    def _(d):
        for step in range(STEPS):
            gather_copy(step, d, me_row).wait_send()
        coef_row_copy(d, me_row).wait_send()

    @pl.loop(1, n_col)
    def _(d):
        for step in range(STEPS):
            scatter_copy(step, col_peer(d), me_col, col_peer(d)).wait_send()
        coef_col_copy(d, me_col).wait_send()


def on_device(tiles, tile_index, tile_count, iterate, basis, coefficients, start_degree):
    n_row = lax.axis_size("row")
    n_col = lax.axis_size("col")
    slots, tile = tiles.shape[2], tiles.shape[-1]
    rows_dev, width = iterate.shape
    block_rows = rows_dev * n_col // tile
    f32, bf16, dma = jnp.float32, jnp.bfloat16, pltpu.SemaphoreType.DMA
    vmem, smem = pltpu.VMEM, pltpu.SMEM
    out = pl.pallas_call(
        functools.partial(kernel, n_row, n_col),
        out_shape=jax.ShapeDtypeStruct((width, rows_dev), f32),
        in_specs=[pl.BlockSpec(memory_space=smem)] * 3
        + [pl.BlockSpec(memory_space=pl.ANY)]
        + [pl.BlockSpec(memory_space=vmem)] * 3,
        out_specs=pl.BlockSpec(memory_space=vmem),
        scratch_shapes=[
            vmem((slots, tile, tile), f32),
            vmem((LEFT, tile, slots * tile), bf16),
            vmem((STEPS, n_row, width, rows_dev), f32),
            vmem((n_row, RIGHT * width, rows_dev), bf16),
            vmem((block_rows * RIGHT * width, slots * tile), bf16),
            vmem((STEPS, n_col, width, rows_dev), f32),
            vmem((STEPS, n_col, width, rows_dev), f32),
            vmem((width, rows_dev), f32),
            vmem((STEPS, width, rows_dev), jnp.int32),
            vmem((width // 2, 2 * STEPS * width), f32),
            vmem((n_col, width // 2, 2 * STEPS * width), f32),
            vmem((width // 2, 2 * STEPS * width), f32),
            vmem((n_row, width // 2, 2 * STEPS * width), f32),
            dma((slots,)),
            dma((STEPS, n_row)),
            dma((STEPS, n_row)),
            dma((STEPS, n_col)),
            dma((STEPS, n_col)),
            dma((n_col,)),
            dma((n_col,)),
            dma((n_row,)),
            dma((n_row,)),
        ],
        compiler_params=pltpu.CompilerParams(
            collective_id=0, has_side_effects=True, vmem_limit_bytes=60 * 2**20
        ),
    )(tile_index[0, 0], tile_count, start_degree, tiles[0, 0], iterate.T, basis.T, coefficients)
    return out.T


def solution(mesh):
    in_specs = (
        P("row", "col", None, None, None),
        P("row", "col", None, None),
        P("row", "col"),
        P(("row", "col"), None),
        P(("row", "col"), None),
        P(("row", "col"), None, None),
        P(),
    )
    out_specs = P(("row", "col"), None)
    return jax.shard_map(
        on_device, mesh=mesh, in_specs=in_specs, out_specs=out_specs, check_vma=False
    )
```

```python
import functools

import jax
import jax.numpy as jnp
from jax import lax
from jax.experimental import pallas as pl
from jax.experimental.pallas import tpu as pltpu
from jax.sharding import PartitionSpec as P

STEPS = 2
PRIME = 16777213
HALF = 8388608.0
MAGIC = 12582912.0
LEFT = 3
RIGHT = 4
MESH = pl.DeviceIdType.MESH


def nearest(value):
    return (value + MAGIC) - MAGIC


def digits(value, bits, count):
    out = []
    for place in range(count - 1, 0, -1):
        top = nearest(value * (2.0 ** (-bits * place)))
        value = value - top * (2.0 ** (bits * place))
        out.append(top)
    out.append(value)
    return out[::-1]


def centred(value):
    return value - jnp.where(value > HALF, float(PRIME), 0.0)


def shrink(value):
    high = (value + 2**23) >> 24
    return value - (high << 24) + 3 * high


def shifted(value, shift):
    if shift == 0:
        return value
    return ((value & (2 ** (24 - shift) - 1)) << shift) + 3 * (value >> (24 - shift))


def kernel(
    n_row, n_col, index_hbm, count_ref, degree_ref, tiles_ref, iterate_hbm, basis_hbm, coef_hbm,
    out_ref, iterate_ref, basis_ref, coef_ref, index_smem, tbuf, abuf, gbuf, lbuf, wbuf, pbuf, rbuf, cur, bterm, csrc, crecv, fsum, frecv,
    small_sem, tile_sem, ag_send, ag_recv, af_send, rs_send, rs_recv, ca_send, ca_recv, cb_send, cb_recv,
):
    me_row = lax.axis_index("row")
    me_col = lax.axis_index("col")
    slots, tile, _ = tiles_ref.shape
    width, rows_dev = iterate_hbm.shape
    per_tile = tile // rows_dev
    block_rows = n_col // per_tile
    band = RIGHT * width

    def row_peer(d):
        return lax.rem(me_row + d, n_row)

    core = lax.rem(me_row, 2)
    chip = lax.div(me_row, 2)
    partner = me_row + 1 - 2 * core

    def chip_peer(k, of_core):
        index, bit = 0, 1
        while bit < n_row // 2:
            index = index + bit * lax.rem(lax.div(chip, bit) + k // bit % 2, 2)
            bit *= 2
        return 2 * index + of_core

    far_first = range(n_row // 2 - 1, 0, -1)
    near_first = sorted(range(1, n_row // 2), key=lambda k: bin(k).count("1"))

    def col_peer(d):
        return lax.rem(me_col + d, n_col)

    small = [
        pltpu.make_async_copy(src, dst, small_sem.at[i])
        for i, (src, dst) in enumerate(
            [
                (iterate_hbm, iterate_ref),
                (coef_hbm, coef_ref),
                (index_hbm, index_smem),
                (basis_hbm, basis_ref),
            ]
        )
    ]
    for load in small:
        load.start()
    loads = [
        pltpu.make_async_copy(tiles_ref.at[t], tbuf.at[t], tile_sem.at[t]) for t in range(slots)
    ]
    for load in loads:
        load.start()

    barrier = pltpu.get_barrier_semaphore()

    @pl.loop(1, n_row)
    def _(d):
        pl.semaphore_signal(barrier, inc=1, device_id={"row": row_peer(d)}, device_id_type=MESH)

    @pl.loop(1, n_col)
    def _(d):
        pl.semaphore_signal(barrier, inc=1, device_id={"col": col_peer(d)}, device_id_type=MESH)

    per_device = coef_hbm.shape[0]
    me = me_row * n_col + me_col
    small[1].wait()
    held = []
    for step in range(STEPS):
        wanted = jnp.broadcast_to(degree_ref[...] - step - me * per_device, (width, width))
        matrix = jnp.where(wanted == 0, coef_ref[0], 0.0)
        for k in range(1, per_device):
            matrix = jnp.where(wanted == k, coef_ref[k], matrix)
        held += [matrix[: width // 2], matrix[width // 2 :]]
    csrc[...] = jnp.concatenate(held, axis=1)

    small[0].wait()
    pl.semaphore_wait(barrier, n_row + n_col - 2)

    def gather_copy(step, peer, slot):
        return pltpu.make_async_remote_copy(
            src_ref=iterate_ref if step == 0 else cur,
            dst_ref=gbuf.at[step, slot],
            send_sem=ag_send.at[step, peer],
            recv_sem=ag_recv.at[step, slot],
            device_id={"row": peer},
            device_id_type=MESH,
        )

    def forward_copy(step, slot):
        return pltpu.make_async_remote_copy(
            src_ref=gbuf.at[step, slot],
            dst_ref=gbuf.at[step, slot],
            send_sem=af_send.at[step, slot],
            recv_sem=ag_recv.at[step, slot],
            device_id={"row": partner},
            device_id_type=MESH,
        )

    def scatter_copy(step, chunk, slot, peer):
        return pltpu.make_async_remote_copy(
            src_ref=pbuf.at[step, chunk],
            dst_ref=rbuf.at[step, slot],
            send_sem=rs_send.at[step, chunk],
            recv_sem=rs_recv.at[step, slot],
            device_id={"col": peer},
            device_id_type=MESH,
        )

    def coef_col_copy(d, slot):
        return pltpu.make_async_remote_copy(
            src_ref=csrc,
            dst_ref=crecv.at[slot],
            send_sem=ca_send.at[d],
            recv_sem=ca_recv.at[slot],
            device_id={"col": col_peer(d)},
            device_id_type=MESH,
        )

    def coef_row_copy(d, slot):
        return pltpu.make_async_remote_copy(
            src_ref=fsum,
            dst_ref=frecv.at[slot],
            send_sem=cb_send.at[d],
            recv_sem=cb_recv.at[slot],
            device_id={"row": row_peer(d)},
            device_id_type=MESH,
        )

    def put_limbs(value, slot):
        parts = digits(centred(value), 6, RIGHT)
        lbuf[slot] = jnp.concatenate(parts, axis=0).astype(jnp.bfloat16)

    def split_tiles():
        rows = 64
        for t in range(slots):
            loads[t].wait()

            @pl.loop(0, tile // rows)
            def _(i, t=t):
                at = pl.ds(pl.multiple_of(i * rows, rows), rows)
                parts = digits(tbuf[t, at, :], 8, LEFT)
                for place in range(LEFT):
                    abuf[place, at, t * tile : (t + 1) * tile] = parts[place].astype(jnp.bfloat16)

    def basis_terms():
        small[3].wait()
        @pl.loop(1, n_row)
        def _(d):
            src = lax.rem(me_row - d + n_row, n_row)
            coef_row_copy(d, src).wait_recv()

        def add(d, total):
            return total + frecv[lax.rem(me_row + d, n_row)]

        coefs = lax.fori_loop(1, n_row, add, fsum[...])
        basis_digits = [x.astype(jnp.bfloat16) for x in digits(centred(basis_ref[...]), 8, 3)]
        for step in range(STEPS):
            low = coefs[:, (2 * step) * width : (2 * step + 1) * width]
            high = coefs[:, (2 * step + 1) * width : (2 * step + 2) * width]
            matrix = centred(jnp.concatenate([low, high], axis=0))
            parts = [x.T.astype(jnp.bfloat16) for x in digits(matrix, 8, 3)]
            left = jnp.concatenate(parts, axis=0)
            sums = [None] * 5
            for place in range(3):
                product = jnp.dot(left, basis_digits[place], preferred_element_type=jnp.float32)
                for other in range(3):
                    piece = product[other * width : (other + 1) * width]
                    old = sums[place + other]
                    sums[place + other] = piece if old is None else old + piece
            sums = [x.astype(jnp.int32) for x in sums]
            total = sums[0] + 3 * sums[3] + ((sums[1] + 3 * sums[4]) << 8)
            total = total + shifted(sums[2], 16)
            bterm[step] = shrink(total)

    for step in range(STEPS):
        if step == 0:

            @pl.loop(1, n_col)
            def _(d):
                coef_col_copy(d, me_col).start()

        for k in far_first:
            gather_copy(step, chip_peer(k, core), me_row).start()
        gather_copy(step, partner, me_row).start()

        put_limbs((iterate_ref if step == 0 else cur)[...], me_row)
        if step == 0:
            split_tiles()

            def add_col(d, total):
                src = lax.rem(me_col - d + n_col, n_col)
                coef_col_copy(d, src).wait_recv()
                return total + crecv[src]

            fsum[...] = lax.fori_loop(1, n_col, add_col, csrc[...])

        for k in near_first:
            src = chip_peer(k, core)
            gather_copy(step, src, src).wait_recv()
            forward_copy(step, src).start()
            put_limbs(gbuf[step, src], src)
        for src in [partner] + [chip_peer(k, 1 - core) for k in near_first]:
            gather_copy(step, partner, src).wait_recv()
            put_limbs(gbuf[step, src], src)

        if step == 0:

            @pl.loop(1, n_row)
            def _(d):
                coef_row_copy(d, me_row).start()

        if step == 0:
            small[2].wait()
        count = jnp.max(count_ref[...])
        for t in range(slots):
            used = t < count
            column = index_smem[1, t]
            for part in range(per_tile):
                window = lbuf[column * per_tile + part]
                at = t * tile + part * rows_dev
                for a in range(block_rows):
                    keep = jnp.where(used & (index_smem[0, t] == a), 1.0, 0.0).astype(jnp.bfloat16)
                    wbuf[a * band : (a + 1) * band, at : at + rows_dev] = window * keep

        for part in range(per_tile):
            rows = slice(part * rows_dev, (part + 1) * rows_dev)
            whole = [
                lax.dot_general(
                    wbuf[...],
                    abuf[place, rows, :],
                    (((1,), (1,)), ((), ())),
                    preferred_element_type=jnp.float32,
                ).astype(jnp.int32)
                for place in range(LEFT)
            ]
            for a in range(block_rows):
                total = None
                for j in range(RIGHT):
                    at = slice(a * band + j * width, a * band + (j + 1) * width)
                    p0, p1, p2 = [x[at] for x in whole]
                    term = p0 + ((p1 & 0xFFFF) << 8) + ((p2 & 0xFF) << 16)
                    term = shifted(term + 3 * ((p1 >> 16) + (p2 >> 8)), 6 * j)
                    total = term if total is None else total + term
                chunk = a * per_tile + part
                pbuf[step, chunk] = shrink(total).astype(jnp.float32)

                @pl.when(me_col != chunk)
                def _(step=step, chunk=chunk):
                    scatter_copy(step, chunk, me_col, chunk).start()

        if step == 0:
            basis_terms()

        def add_chunk(d, total, step=step):
            src = lax.rem(me_col - d + n_col, n_col)
            scatter_copy(step, src, src, src).wait_recv()
            return total + rbuf[step, src].astype(jnp.int32)

        start = bterm[step] + pbuf[step, me_col].astype(jnp.int32)
        value = shrink(lax.fori_loop(1, n_col, add_chunk, start))
        if step < STEPS - 1:
            cur[...] = value.astype(jnp.float32)
        else:
            value = jnp.where(value < 0, value + PRIME, value)
            out_ref[...] = value.astype(jnp.float32) / float(PRIME)

    for step in range(STEPS):
        gather_copy(step, partner, me_row).wait_send()
        for k in near_first:
            gather_copy(step, chip_peer(k, core), me_row).wait_send()
            forward_copy(step, chip_peer(k, core)).wait_send()

    @pl.loop(1, n_row)
    def _(d):
        coef_row_copy(d, me_row).wait_send()

    @pl.loop(1, n_col)
    def _(d):
        for step in range(STEPS):
            scatter_copy(step, col_peer(d), me_col, col_peer(d)).wait_send()
        coef_col_copy(d, me_col).wait_send()


def on_device(tiles, tile_index, tile_count, iterate, basis, coefficients, start_degree):
    n_row = lax.axis_size("row")
    n_col = lax.axis_size("col")
    slots, tile = tiles.shape[2], tiles.shape[-1]
    rows_dev, width = iterate.shape
    block_rows = rows_dev * n_col // tile
    f32, bf16, dma = jnp.float32, jnp.bfloat16, pltpu.SemaphoreType.DMA
    vmem, smem = pltpu.VMEM, pltpu.SMEM
    out = pl.pallas_call(
        functools.partial(kernel, n_row, n_col),
        out_shape=jax.ShapeDtypeStruct((width, rows_dev), f32),
        in_specs=[
            pl.BlockSpec(memory_space=space)
            for space in (pl.ANY, vmem, vmem, pl.ANY, pl.ANY, pl.ANY, pl.ANY)
        ],
        out_specs=pl.BlockSpec(memory_space=vmem),
        scratch_shapes=[
            vmem((width, rows_dev), f32),
            vmem((width, rows_dev), f32),
            vmem(coefficients.shape, f32),
            smem((2, slots), jnp.int32),
            vmem((slots, tile, tile), f32),
            vmem((LEFT, tile, slots * tile), bf16),
            vmem((STEPS, n_row, width, rows_dev), f32),
            vmem((n_row, RIGHT * width, rows_dev), bf16),
            vmem((block_rows * RIGHT * width, slots * tile), bf16),
            vmem((STEPS, n_col, width, rows_dev), f32),
            vmem((STEPS, n_col, width, rows_dev), f32),
            vmem((width, rows_dev), f32),
            vmem((STEPS, width, rows_dev), jnp.int32),
            vmem((width // 2, 2 * STEPS * width), f32),
            vmem((n_col, width // 2, 2 * STEPS * width), f32),
            vmem((width // 2, 2 * STEPS * width), f32),
            vmem((n_row, width // 2, 2 * STEPS * width), f32),
            dma((4,)),
            dma((slots,)),
            dma((STEPS, n_row)),
            dma((STEPS, n_row)),
            dma((STEPS, n_row)),
            dma((STEPS, n_col)),
            dma((STEPS, n_col)),
            dma((n_col,)),
            dma((n_col,)),
            dma((n_row,)),
            dma((n_row,)),
        ],
        compiler_params=pltpu.CompilerParams(
            collective_id=0, has_side_effects=True, vmem_limit_bytes=60 * 2**20
        ),
    )(tile_index[0, 0].T, tile_count, start_degree.reshape(1, 1), tiles[0, 0], iterate.T, basis.T, coefficients)
    return out.T


def solution(mesh):
    in_specs = (
        P("row", "col", None, None, None),
        P("row", "col", None, None),
        P("row", "col"),
        P(("row", "col"), None),
        P(("row", "col"), None),
        P(("row", "col"), None, None),
        P(),
    )
    out_specs = P(("row", "col"), None)
    return jax.shard_map(
        on_device, mesh=mesh, in_specs=in_specs, out_specs=out_specs, check_vma=False
    )
```

```python
import functools

import jax
import jax.numpy as jnp
from jax import lax
from jax.experimental import pallas as pl
from jax.experimental.pallas import tpu as pltpu
from jax.sharding import PartitionSpec as P

STEPS = 2
PRIME = 16777213
HALF = 8388608.0
MAGIC = 12582912.0
LEFT = 3
RIGHT = 4
MESH = pl.DeviceIdType.MESH


def nearest(value):
    return (value + MAGIC) - MAGIC


def digits(value, bits, count):
    out = []
    for place in range(count - 1, 0, -1):
        top = nearest(value * (2.0 ** (-bits * place)))
        value = value - top * (2.0 ** (bits * place))
        out.append(top)
    out.append(value)
    return out[::-1]


def centred(value):
    return value - jnp.where(value > HALF, float(PRIME), 0.0)


def shrink(value):
    high = (value + 2**23) >> 24
    return value - (high << 24) + 3 * high


def shifted(value, shift):
    if shift == 0:
        return value
    return ((value & (2 ** (24 - shift) - 1)) << shift) + 3 * (value >> (24 - shift))


def kernel(
    n_row, n_col, index_hbm, count_ref, degree_ref, tiles_ref, iterate_hbm, basis_hbm, coef_hbm,
    out_ref, iterate_ref, basis_ref, coef_ref, index_smem, tbuf, abuf, gbuf, lbuf, wbuf, pbuf,
    rbuf, cur, bterm, csrc, crecv, fsum, frecv, small_sem, tile_sem, ag_send, ag_recv, af_send,
    rs_send, rs_recv, ca_send, ca_recv, cb_send, cb_recv,
):
    me_row = lax.axis_index("row")
    me_col = lax.axis_index("col")
    slots, tile, _ = tiles_ref.shape
    width, rows_dev = iterate_hbm.shape
    per_tile = tile // rows_dev
    block_rows = n_col // per_tile
    band = RIGHT * width

    def row_peer(d):
        return lax.rem(me_row + d, n_row)

    core = lax.rem(me_row, 2)
    chip = lax.div(me_row, 2)
    partner = me_row + 1 - 2 * core

    def chip_peer(k, of_core):
        index, bit = 0, 1
        while bit < n_row // 2:
            index = index + bit * lax.rem(lax.div(chip, bit) + k // bit % 2, 2)
            bit *= 2
        return 2 * index + of_core

    far_first = range(n_row // 2 - 1, 0, -1)
    near_first = sorted(range(1, n_row // 2), key=lambda k: bin(k).count("1"))

    def col_peer(d):
        return lax.rem(me_col + d, n_col)

    small = [
        pltpu.make_async_copy(src, dst, small_sem.at[i])
        for i, (src, dst) in enumerate(
            [
                (iterate_hbm, iterate_ref),
                (coef_hbm, coef_ref),
                (index_hbm, index_smem),
                (basis_hbm, basis_ref),
            ]
        )
    ]
    for load in small:
        load.start()
    loads = [
        pltpu.make_async_copy(tiles_ref.at[t], tbuf.at[t], tile_sem.at[t]) for t in range(slots)
    ]
    for load in loads:
        load.start()

    barrier = pltpu.get_barrier_semaphore()

    @pl.loop(1, n_row)
    def _(d):
        pl.semaphore_signal(barrier, inc=1, device_id={"row": row_peer(d)}, device_id_type=MESH)

    @pl.loop(1, n_col)
    def _(d):
        pl.semaphore_signal(barrier, inc=1, device_id={"col": col_peer(d)}, device_id_type=MESH)

    per_device = coef_hbm.shape[0]
    me = me_row * n_col + me_col
    small[1].wait()
    held = []
    for step in range(STEPS):
        wanted = jnp.broadcast_to(degree_ref[...] - step - me * per_device, (width, width))
        matrix = jnp.where(wanted == 0, coef_ref[0], 0.0)
        for k in range(1, per_device):
            matrix = jnp.where(wanted == k, coef_ref[k], matrix)
        held += [matrix[: width // 2], matrix[width // 2 :]]
    csrc[...] = jnp.concatenate(held, axis=1)

    small[0].wait()
    pl.semaphore_wait(barrier, n_row + n_col - 2)

    def gather_copy(step, peer, slot):
        return pltpu.make_async_remote_copy(
            src_ref=iterate_ref if step == 0 else cur,
            dst_ref=gbuf.at[step, slot],
            send_sem=ag_send.at[step, peer],
            recv_sem=ag_recv.at[step, slot],
            device_id={"row": peer},
            device_id_type=MESH,
        )

    def forward_copy(step, slot):
        return pltpu.make_async_remote_copy(
            src_ref=gbuf.at[step, slot],
            dst_ref=gbuf.at[step, slot],
            send_sem=af_send.at[step, slot],
            recv_sem=ag_recv.at[step, slot],
            device_id={"row": partner},
            device_id_type=MESH,
        )

    def scatter_copy(step, chunk, slot, peer):
        return pltpu.make_async_remote_copy(
            src_ref=pbuf.at[step, chunk],
            dst_ref=rbuf.at[step, slot],
            send_sem=rs_send.at[step, chunk],
            recv_sem=rs_recv.at[step, slot],
            device_id={"col": peer},
            device_id_type=MESH,
        )

    def coef_col_copy(d, slot):
        return pltpu.make_async_remote_copy(
            src_ref=csrc,
            dst_ref=crecv.at[slot],
            send_sem=ca_send.at[d],
            recv_sem=ca_recv.at[slot],
            device_id={"col": col_peer(d)},
            device_id_type=MESH,
        )

    def coef_row_copy(d, slot):
        return pltpu.make_async_remote_copy(
            src_ref=fsum,
            dst_ref=frecv.at[slot],
            send_sem=cb_send.at[d],
            recv_sem=cb_recv.at[slot],
            device_id={"row": row_peer(d)},
            device_id_type=MESH,
        )

    def put_limbs(value, slot):
        parts = digits(centred(value), 6, RIGHT)
        lbuf[slot] = jnp.concatenate(parts, axis=0).astype(jnp.bfloat16)

    def split_tiles():
        rows = 64
        for t in range(slots):
            loads[t].wait()

            @pl.loop(0, tile // rows)
            def _(i, t=t):
                at = pl.ds(pl.multiple_of(i * rows, rows), rows)
                parts = digits(tbuf[t, at, :], 8, LEFT)
                for place in range(LEFT):
                    abuf[place, at, t * tile : (t + 1) * tile] = parts[place].astype(jnp.bfloat16)

    def basis_terms():
        small[3].wait()
        @pl.loop(1, n_row)
        def _(d):
            src = lax.rem(me_row - d + n_row, n_row)
            coef_row_copy(d, src).wait_recv()

        def add(d, total):
            return total + frecv[lax.rem(me_row + d, n_row)]

        coefs = lax.fori_loop(1, n_row, add, fsum[...])
        basis_digits = [x.astype(jnp.bfloat16) for x in digits(centred(basis_ref[...]), 8, 3)]
        for step in range(STEPS):
            low = coefs[:, (2 * step) * width : (2 * step + 1) * width]
            high = coefs[:, (2 * step + 1) * width : (2 * step + 2) * width]
            matrix = centred(jnp.concatenate([low, high], axis=0))
            parts = [x.T.astype(jnp.bfloat16) for x in digits(matrix, 8, 3)]
            left = jnp.concatenate(parts, axis=0)
            sums = [None] * 5
            for place in range(3):
                product = jnp.dot(left, basis_digits[place], preferred_element_type=jnp.float32)
                for other in range(3):
                    piece = product[other * width : (other + 1) * width]
                    old = sums[place + other]
                    sums[place + other] = piece if old is None else old + piece
            sums = [x.astype(jnp.int32) for x in sums]
            total = sums[0] + 3 * sums[3] + ((sums[1] + 3 * sums[4]) << 8)
            total = total + shifted(sums[2], 16)
            bterm[step] = shrink(total)

    for step in range(STEPS):
        if step == 0:

            @pl.loop(1, n_col)
            def _(d):
                coef_col_copy(d, me_col).start()

        for k in far_first:
            gather_copy(step, chip_peer(k, core), me_row).start()
        gather_copy(step, partner, me_row).start()

        put_limbs((iterate_ref if step == 0 else cur)[...], me_row)
        if step == 0:
            split_tiles()

            def add_col(d, total):
                src = lax.rem(me_col - d + n_col, n_col)
                coef_col_copy(d, src).wait_recv()
                return total + crecv[src]

            fsum[...] = lax.fori_loop(1, n_col, add_col, csrc[...])

        for k in near_first:
            src = chip_peer(k, core)
            gather_copy(step, src, src).wait_recv()
            forward_copy(step, src).start()
            put_limbs(gbuf[step, src], src)
        for src in [partner] + [chip_peer(k, 1 - core) for k in near_first]:
            gather_copy(step, partner, src).wait_recv()
            put_limbs(gbuf[step, src], src)

        if step == 0:

            @pl.loop(1, n_row)
            def _(d):
                coef_row_copy(d, me_row).start()

        if step == 0:
            small[2].wait()
        count = jnp.max(count_ref[...])
        for t in range(slots):
            used = t < count
            column = index_smem[1, t]
            for part in range(per_tile):
                window = lbuf[column * per_tile + part]
                at = t * tile + part * rows_dev
                for a in range(block_rows):
                    keep = jnp.where(used & (index_smem[0, t] == a), 1.0, 0.0).astype(jnp.bfloat16)
                    wbuf[a * band : (a + 1) * band, at : at + rows_dev] = window * keep

        for part in range(per_tile):
            rows = slice(part * rows_dev, (part + 1) * rows_dev)
            whole = [
                lax.dot_general(
                    wbuf[...],
                    abuf[place, rows, :],
                    (((1,), (1,)), ((), ())),
                    preferred_element_type=jnp.float32,
                ).astype(jnp.int32)
                for place in range(LEFT)
            ]
            for a in range(block_rows):
                total = None
                for j in range(RIGHT):
                    at = slice(a * band + j * width, a * band + (j + 1) * width)
                    p0, p1, p2 = [x[at] for x in whole]
                    term = p0 + ((p1 & 0xFFFF) << 8) + ((p2 & 0xFF) << 16)
                    term = shifted(term + 3 * ((p1 >> 16) + (p2 >> 8)), 6 * j)
                    total = term if total is None else total + term
                chunk = a * per_tile + part
                pbuf[step, chunk] = shrink(total).astype(jnp.float32)

                @pl.when(me_col != chunk)
                def _(step=step, chunk=chunk):
                    scatter_copy(step, chunk, me_col, chunk).start()

        if step == 0:
            basis_terms()

        def add_chunk(d, total, step=step):
            src = lax.rem(me_col - d + n_col, n_col)
            scatter_copy(step, src, src, src).wait_recv()
            return total + rbuf[step, src].astype(jnp.int32)

        start = bterm[step] + pbuf[step, me_col].astype(jnp.int32)
        value = shrink(lax.fori_loop(1, n_col, add_chunk, start))
        if step < STEPS - 1:
            cur[...] = value.astype(jnp.float32)
        else:
            value = jnp.where(value < 0, value + PRIME, value)
            out_ref[...] = value.astype(jnp.float32) / float(PRIME)

    for step in range(STEPS):
        gather_copy(step, partner, me_row).wait_send()
        for k in near_first:
            gather_copy(step, chip_peer(k, core), me_row).wait_send()
            forward_copy(step, chip_peer(k, core)).wait_send()

    @pl.loop(1, n_row)
    def _(d):
        coef_row_copy(d, me_row).wait_send()

    @pl.loop(1, n_col)
    def _(d):
        for step in range(STEPS):
            scatter_copy(step, col_peer(d), me_col, col_peer(d)).wait_send()
        coef_col_copy(d, me_col).wait_send()


def on_device(tiles, tile_index, tile_count, iterate, basis, coefficients, start_degree):
    n_row = lax.axis_size("row")
    n_col = lax.axis_size("col")
    slots, tile = tiles.shape[2], tiles.shape[-1]
    rows_dev, width = iterate.shape
    block_rows = rows_dev * n_col // tile
    f32, bf16, dma = jnp.float32, jnp.bfloat16, pltpu.SemaphoreType.DMA
    vmem, smem = pltpu.VMEM, pltpu.SMEM
    out = pl.pallas_call(
        functools.partial(kernel, n_row, n_col),
        out_shape=vmem((width, rows_dev), f32),
        in_specs=[
            pl.BlockSpec(memory_space=space)
            for space in (pl.ANY, vmem, vmem, pl.ANY, pl.ANY, pl.ANY, pl.ANY)
        ],
        out_specs=pl.BlockSpec(memory_space=vmem),
        scratch_shapes=[
            vmem((width, rows_dev), f32),
            vmem((width, rows_dev), f32),
            vmem(coefficients.shape, f32),
            smem((2, slots), jnp.int32),
            vmem((slots, tile, tile), f32),
            vmem((LEFT, tile, slots * tile), bf16),
            vmem((STEPS, n_row, width, rows_dev), f32),
            vmem((n_row, RIGHT * width, rows_dev), bf16),
            vmem((block_rows * RIGHT * width, slots * tile), bf16),
            vmem((STEPS, n_col, width, rows_dev), f32),
            vmem((STEPS, n_col, width, rows_dev), f32),
            vmem((width, rows_dev), f32),
            vmem((STEPS, width, rows_dev), jnp.int32),
            vmem((width // 2, 2 * STEPS * width), f32),
            vmem((n_col, width // 2, 2 * STEPS * width), f32),
            vmem((width // 2, 2 * STEPS * width), f32),
            vmem((n_row, width // 2, 2 * STEPS * width), f32),
            dma((4,)),
            dma((slots,)),
            dma((STEPS, n_row)),
            dma((STEPS, n_row)),
            dma((STEPS, n_row)),
            dma((STEPS, n_col)),
            dma((STEPS, n_col)),
            dma((n_col,)),
            dma((n_col,)),
            dma((n_row,)),
            dma((n_row,)),
        ],
        compiler_params=pltpu.CompilerParams(
            collective_id=0, has_side_effects=True, vmem_limit_bytes=60 * 2**20
        ),
    )(tile_index[0, 0].T, tile_count, start_degree.reshape(1, 1), tiles[0, 0], iterate.T, basis.T, coefficients)
    return out.T


def solution(mesh):
    in_specs = (
        P("row", "col", None, None, None),
        P("row", "col", None, None),
        P("row", "col"),
        P(("row", "col"), None),
        P(("row", "col"), None),
        P(("row", "col"), None, None),
        P(),
    )
    out_specs = P(("row", "col"), None)
    return jax.shard_map(
        on_device, mesh=mesh, in_specs=in_specs, out_specs=out_specs, check_vma=False
    )
```

```python
import functools

import jax
import jax.numpy as jnp
from jax import lax
from jax.experimental import pallas as pl
from jax.experimental.pallas import tpu as pltpu
from jax.sharding import PartitionSpec as P

STEPS = 2
PRIME = 16777213
HALF = 8388608.0
MAGIC = 12582912.0
LEFT = 3
RIGHT = 4
MESH = pl.DeviceIdType.MESH


def nearest(value):
    return (value + MAGIC) - MAGIC


def digits(value, bits, count):
    out = []
    for place in range(count - 1, 0, -1):
        top = nearest(value * (2.0 ** (-bits * place)))
        value = value - top * (2.0 ** (bits * place))
        out.append(top)
    out.append(value)
    return out[::-1]


def centred(value):
    return value - jnp.where(value > HALF, float(PRIME), 0.0)


def shrink(value):
    high = (value + 2**23) >> 24
    return value - (high << 24) + 3 * high


def shifted(value, shift):
    if shift == 0:
        return value
    return ((value & (2 ** (24 - shift) - 1)) << shift) + 3 * (value >> (24 - shift))


def kernel(
    n_row, n_col, index_hbm, count_ref, degree_ref, tiles_ref, iterate_hbm, basis_hbm, coef_hbm,
    out_ref, iterate_ref, basis_ref, coef_ref, index_smem, tbuf, abuf, gbuf, lbuf, wbuf, pbuf,
    rbuf, cur, bterm, csrc, crecv, fsum, frecv, small_sem, tile_sem, ag_send, ag_recv, af_send,
    rs_send, rs_recv, ca_send, ca_recv, cb_send, cb_recv,
):
    me_row = lax.axis_index("row")
    me_col = lax.axis_index("col")
    slots, tile, _ = tiles_ref.shape
    width, rows_dev = iterate_hbm.shape
    per_tile = tile // rows_dev
    block_rows = n_col // per_tile
    band = RIGHT * width

    def row_peer(d):
        return lax.rem(me_row + d, n_row)

    core = lax.rem(me_row, 2)
    chip = lax.div(me_row, 2)
    partner = me_row + 1 - 2 * core

    def chip_peer(k, of_core):
        index, bit = 0, 1
        while bit < n_row // 2:
            index = index + bit * lax.rem(lax.div(chip, bit) + k // bit % 2, 2)
            bit *= 2
        return 2 * index + of_core

    far_first = range(n_row // 2 - 1, 0, -1)
    near_first = sorted(range(1, n_row // 2), key=lambda k: bin(k).count("1"))

    def col_peer(d):
        return lax.rem(me_col + d, n_col)

    small = [
        pltpu.make_async_copy(src, dst, small_sem.at[i])
        for i, (src, dst) in enumerate(
            [
                (iterate_hbm, iterate_ref),
                (coef_hbm, coef_ref),
                (index_hbm, index_smem),
                (basis_hbm, basis_ref),
            ]
        )
    ]
    for load in small:
        load.start()
    loads = [
        pltpu.make_async_copy(tiles_ref.at[t], tbuf.at[t], tile_sem.at[t]) for t in range(slots)
    ]
    for load in loads:
        load.start()

    barrier = pltpu.get_barrier_semaphore()

    @pl.loop(1, n_row)
    def _(d):
        pl.semaphore_signal(barrier, inc=1, device_id={"row": row_peer(d)}, device_id_type=MESH)

    @pl.loop(1, n_col)
    def _(d):
        pl.semaphore_signal(barrier, inc=1, device_id={"col": col_peer(d)}, device_id_type=MESH)

    per_device = coef_hbm.shape[0]
    me = me_row * n_col + me_col
    small[1].wait()
    held = []
    for step in range(STEPS):
        wanted = jnp.broadcast_to(degree_ref[...] - step - me * per_device, (width, width))
        matrix = jnp.where(wanted == 0, coef_ref[0], 0.0)
        for k in range(1, per_device):
            matrix = jnp.where(wanted == k, coef_ref[k], matrix)
        held += [matrix[: width // 2], matrix[width // 2 :]]
    csrc[...] = jnp.concatenate(held, axis=1)

    small[0].wait()
    pl.semaphore_wait(barrier, n_row + n_col - 2)

    def gather_copy(step, peer, slot):
        return pltpu.make_async_remote_copy(
            src_ref=iterate_ref if step == 0 else cur,
            dst_ref=gbuf.at[step, slot],
            send_sem=ag_send.at[step, peer],
            recv_sem=ag_recv.at[step, slot],
            device_id={"row": peer},
            device_id_type=MESH,
        )

    def forward_copy(step, slot):
        return pltpu.make_async_remote_copy(
            src_ref=gbuf.at[step, slot],
            dst_ref=gbuf.at[step, slot],
            send_sem=af_send.at[step, slot],
            recv_sem=ag_recv.at[step, slot],
            device_id={"row": partner},
            device_id_type=MESH,
        )

    def scatter_copy(step, chunk, slot, peer):
        return pltpu.make_async_remote_copy(
            src_ref=pbuf.at[step, chunk],
            dst_ref=rbuf.at[step, slot],
            send_sem=rs_send.at[step, chunk],
            recv_sem=rs_recv.at[step, slot],
            device_id={"col": peer},
            device_id_type=MESH,
        )

    def coef_col_copy(d, slot):
        return pltpu.make_async_remote_copy(
            src_ref=csrc,
            dst_ref=crecv.at[slot],
            send_sem=ca_send.at[d],
            recv_sem=ca_recv.at[slot],
            device_id={"col": col_peer(d)},
            device_id_type=MESH,
        )

    def coef_row_copy(d, slot):
        return pltpu.make_async_remote_copy(
            src_ref=fsum,
            dst_ref=frecv.at[slot],
            send_sem=cb_send.at[d],
            recv_sem=cb_recv.at[slot],
            device_id={"row": row_peer(d)},
            device_id_type=MESH,
        )

    def put_limbs(value, slot):
        parts = digits(centred(value), 6, RIGHT)
        lbuf[slot] = jnp.concatenate(parts, axis=0).astype(jnp.bfloat16)

    def split_tiles():
        rows = 64
        for t in range(slots):
            loads[t].wait()

            @pl.loop(0, tile // rows)
            def _(i, t=t):
                at = pl.ds(pl.multiple_of(i * rows, rows), rows)
                parts = digits(tbuf[t, at, :], 8, LEFT)
                for place in range(LEFT):
                    abuf[place, at, t * tile : (t + 1) * tile] = parts[place].astype(jnp.bfloat16)

    def basis_terms():
        small[3].wait()
        @pl.loop(1, n_row)
        def _(d):
            src = lax.rem(me_row - d + n_row, n_row)
            coef_row_copy(d, src).wait_recv()

        def add(d, total):
            return total + frecv[lax.rem(me_row + d, n_row)]

        coefs = lax.fori_loop(1, n_row, add, fsum[...])
        basis_digits = [x.astype(jnp.bfloat16) for x in digits(centred(basis_ref[...]), 8, 3)]
        for step in range(STEPS):
            low = coefs[:, (2 * step) * width : (2 * step + 1) * width]
            high = coefs[:, (2 * step + 1) * width : (2 * step + 2) * width]
            matrix = centred(jnp.concatenate([low, high], axis=0))
            parts = [x.T.astype(jnp.bfloat16) for x in digits(matrix, 8, 3)]
            left = jnp.concatenate(parts, axis=0)
            sums = [None] * 5
            for place in range(3):
                product = jnp.dot(left, basis_digits[place], preferred_element_type=jnp.float32)
                for other in range(3):
                    piece = product[other * width : (other + 1) * width]
                    old = sums[place + other]
                    sums[place + other] = piece if old is None else old + piece
            sums = [x.astype(jnp.int32) for x in sums]
            total = sums[0] + 3 * sums[3] + ((sums[1] + 3 * sums[4]) << 8)
            total = total + shifted(sums[2], 16)
            bterm[step] = shrink(total)

    for step in range(STEPS):
        if step == 0:

            @pl.loop(1, n_col)
            def _(d):
                coef_col_copy(d, me_col).start()

        for k in far_first:
            gather_copy(step, chip_peer(k, core), me_row).start()
        gather_copy(step, partner, me_row).start()

        put_limbs((iterate_ref if step == 0 else cur)[...], me_row)
        if step == 0:
            split_tiles()

        for k in near_first:
            src = chip_peer(k, core)
            gather_copy(step, src, src).wait_recv()
            forward_copy(step, src).start()
            put_limbs(gbuf[step, src], src)
        for src in [partner] + [chip_peer(k, 1 - core) for k in near_first]:
            gather_copy(step, partner, src).wait_recv()
            put_limbs(gbuf[step, src], src)

        if step == 0:

            def add_col(d, total):
                src = lax.rem(me_col - d + n_col, n_col)
                coef_col_copy(d, src).wait_recv()
                return total + crecv[src]

            fsum[...] = lax.fori_loop(1, n_col, add_col, csrc[...])

            @pl.loop(1, n_row)
            def _(d):
                coef_row_copy(d, me_row).start()

        if step == 0:
            small[2].wait()
        count = jnp.max(count_ref[...])
        for t in range(slots):
            used = t < count
            column = index_smem[1, t]
            for part in range(per_tile):
                window = lbuf[column * per_tile + part]
                at = t * tile + part * rows_dev
                for a in range(block_rows):
                    keep = jnp.where(used & (index_smem[0, t] == a), 1.0, 0.0).astype(jnp.bfloat16)
                    wbuf[a * band : (a + 1) * band, at : at + rows_dev] = window * keep

        for part in range(per_tile):
            rows = slice(part * rows_dev, (part + 1) * rows_dev)
            whole = [
                lax.dot_general(
                    wbuf[...],
                    abuf[place, rows, :],
                    (((1,), (1,)), ((), ())),
                    preferred_element_type=jnp.float32,
                ).astype(jnp.int32)
                for place in range(LEFT)
            ]
            for a in range(block_rows):
                total = None
                for j in range(RIGHT):
                    at = slice(a * band + j * width, a * band + (j + 1) * width)
                    p0, p1, p2 = [x[at] for x in whole]
                    term = p0 + ((p1 & 0xFFFF) << 8) + ((p2 & 0xFF) << 16)
                    term = shifted(term + 3 * ((p1 >> 16) + (p2 >> 8)), 6 * j)
                    total = term if total is None else total + term
                chunk = a * per_tile + part
                pbuf[step, chunk] = shrink(total).astype(jnp.float32)

                @pl.when(me_col != chunk)
                def _(step=step, chunk=chunk):
                    scatter_copy(step, chunk, me_col, chunk).start()

        if step == 0:
            basis_terms()

        def add_chunk(d, total, step=step):
            src = lax.rem(me_col - d + n_col, n_col)
            scatter_copy(step, src, src, src).wait_recv()
            return total + rbuf[step, src].astype(jnp.int32)

        start = bterm[step] + pbuf[step, me_col].astype(jnp.int32)
        value = shrink(lax.fori_loop(1, n_col, add_chunk, start))
        if step < STEPS - 1:
            cur[...] = value.astype(jnp.float32)
        else:
            value = jnp.where(value < 0, value + PRIME, value)
            out_ref[...] = value.astype(jnp.float32) / float(PRIME)

    for step in range(STEPS):
        gather_copy(step, partner, me_row).wait_send()
        for k in near_first:
            gather_copy(step, chip_peer(k, core), me_row).wait_send()
            forward_copy(step, chip_peer(k, core)).wait_send()

    @pl.loop(1, n_row)
    def _(d):
        coef_row_copy(d, me_row).wait_send()

    @pl.loop(1, n_col)
    def _(d):
        for step in range(STEPS):
            scatter_copy(step, col_peer(d), me_col, col_peer(d)).wait_send()
        coef_col_copy(d, me_col).wait_send()


def on_device(tiles, tile_index, tile_count, iterate, basis, coefficients, start_degree):
    n_row = lax.axis_size("row")
    n_col = lax.axis_size("col")
    slots, tile = tiles.shape[2], tiles.shape[-1]
    rows_dev, width = iterate.shape
    block_rows = rows_dev * n_col // tile
    f32, bf16, dma = jnp.float32, jnp.bfloat16, pltpu.SemaphoreType.DMA
    vmem, smem = pltpu.VMEM, pltpu.SMEM
    out = pl.pallas_call(
        functools.partial(kernel, n_row, n_col),
        out_shape=vmem((width, rows_dev), f32),
        in_specs=[
            pl.BlockSpec(memory_space=space)
            for space in (pl.ANY, vmem, vmem, pl.ANY, pl.ANY, pl.ANY, pl.ANY)
        ],
        out_specs=pl.BlockSpec(memory_space=vmem),
        scratch_shapes=[
            vmem((width, rows_dev), f32),
            vmem((width, rows_dev), f32),
            vmem(coefficients.shape, f32),
            smem((2, slots), jnp.int32),
            vmem((slots, tile, tile), f32),
            vmem((LEFT, tile, slots * tile), bf16),
            vmem((STEPS, n_row, width, rows_dev), f32),
            vmem((n_row, RIGHT * width, rows_dev), bf16),
            vmem((block_rows * RIGHT * width, slots * tile), bf16),
            vmem((STEPS, n_col, width, rows_dev), f32),
            vmem((STEPS, n_col, width, rows_dev), f32),
            vmem((width, rows_dev), f32),
            vmem((STEPS, width, rows_dev), jnp.int32),
            vmem((width // 2, 2 * STEPS * width), f32),
            vmem((n_col, width // 2, 2 * STEPS * width), f32),
            vmem((width // 2, 2 * STEPS * width), f32),
            vmem((n_row, width // 2, 2 * STEPS * width), f32),
            dma((4,)),
            dma((slots,)),
            dma((STEPS, n_row)),
            dma((STEPS, n_row)),
            dma((STEPS, n_row)),
            dma((STEPS, n_col)),
            dma((STEPS, n_col)),
            dma((n_col,)),
            dma((n_col,)),
            dma((n_row,)),
            dma((n_row,)),
        ],
        compiler_params=pltpu.CompilerParams(
            collective_id=0, has_side_effects=True, vmem_limit_bytes=60 * 2**20
        ),
    )(tile_index[0, 0].T, tile_count, start_degree.reshape(1, 1), tiles[0, 0], iterate.T, basis.T, coefficients)
    return out.T


def solution(mesh):
    in_specs = (
        P("row", "col", None, None, None),
        P("row", "col", None, None),
        P("row", "col"),
        P(("row", "col"), None),
        P(("row", "col"), None),
        P(("row", "col"), None, None),
        P(),
    )
    out_specs = P(("row", "col"), None)
    return jax.shard_map(
        on_device, mesh=mesh, in_specs=in_specs, out_specs=out_specs, check_vma=False
    )
```
